32 devices in a mesh: gx: 8 (over z, y), gy: 4 (over x, core).
Axes of the slice: x: 2, y: 2, z: 4, core: 2. Of those that a mesh axis runs over, the one named last changes fastest.
Arguments:
- rhs: bfloat16 [512, 32768], P(None, ('gy', 'gx')), may hold values from -6 to 6
- leaf_inverse: bfloat16 [32, 1024, 1024], P(('gy', 'gx')), may hold values from -0.1875 to 0.1875
- up_basis: bfloat16 [5, 128, 32768], P(None, None, ('gy', 'gx')), may hold values from -0.25 to 0.25
- projection: bfloat16 [5, 256, 32768], P(None, None, ('gy', 'gx')), may hold values from -0.13258252 to 0.13258252, as said below
Outputs:
- solution: float32 [512, 32768], P(None, ('gy', 'gx'))
The draws below stay inside these ranges and needn't reach their ends.
Inputs may be any that keep to these rules, and one draw needn't show every extreme that they name: `projection`: rows of level h (counted from 1) have entries of order (2^h * 1024)^(-1/2).
All inputs are finite; a program needn't handle non-finite values.
Results may differ from the reference program's by a relative error of at most 0.0095.
Values sent between devices are 32-bit elements; how exact they have to be, the bound alone decides.
A program may use at most 64 MiB of HBM per device.

```python
import jax
import jax.numpy as jnp
from jax import lax

LEAF = 1024
RANK = 128
RHS = 512
LEVELS = 5
POINTS = 32768


def draw_projection(key, part):
    heights = jnp.arange(1, LEVELS + 1).astype(jnp.float32)
    scales = 1.0 / jnp.sqrt(LEAF * 2.0 ** heights)
    values = jnp.clip(jax.random.normal(key, (LEVELS, 2 * RANK, POINTS), jnp.float32), -6.0, 6.0)
    return (values * scales[:, None, None]).astype(jnp.bfloat16)


def shard_levels(rng, shape, pieces, least, high):
    level, own = 1.0, jax.random.fold_in(rng, 6)
    for position, shards_of in pieces:
        draws = jnp.exp(jax.random.uniform(jax.random.fold_in(own, position), (shards_of,), jnp.float32, least / len(pieces), high / len(pieces)))
        level = level * jnp.repeat(draws, shape[position] // shards_of).reshape([-1 if axis == position else 1 for axis in range(len(shape))])
    return level


def gaussian(key, dims, deviation, limit, shards=(), dtype=jnp.bfloat16):
    factor_of = shard_levels(key, dims, shards, -0.22, 0.18) if shards else 1.0
    array = jax.random.normal(key, dims, jnp.float32) * deviation * factor_of
    return jnp.minimum(jnp.maximum(array, -limit), limit).astype(dtype)


def setup_inputs(seed: int = 0) -> dict:
    arg_keys = jax.random.split(jax.random.key(seed), 5)
    return {
        "rhs": gaussian(arg_keys[0], (RHS, POINTS), 1.0, 6.0, ((1, 32),)),
        "leaf_inverse": gaussian(arg_keys[1], (POINTS // LEAF, LEAF, LEAF), LEAF ** -0.5, 0.1875, ((0, 32),)),
        "up_basis": gaussian(arg_keys[2], (LEVELS, RANK, POINTS), (4 * RANK) ** -0.5, 0.25, ((2, 32),)),
        "projection": draw_projection(jax.random.fold_in(arg_keys[4], 71), 0),
    }


def leaf_apply(operands):
    return jnp.dot(operands[0], operands[1], preferred_element_type=jnp.float32)


def project_leaf(operands):
    return lax.dot_general(operands[0], operands[1], (((1,), (1,)), ((), ())), preferred_element_type=jnp.float32)


def reference(rhs, leaf_inverse, up_basis, projection):
    leaves = leaf_inverse.shape[0]
    blocks = rhs.reshape(RHS, leaves, LEAF).transpose(1, 0, 2)
    state = lax.map(leaf_apply, (blocks, leaf_inverse))
    for height in range(1, LEVELS + 1):
        rounded = state.astype(jnp.bfloat16)
        basis_rows = projection[height - 1].reshape(2 * RANK, leaves, LEAF).transpose(1, 0, 2)
        up_rows = up_basis[height - 1].reshape(RANK, leaves, LEAF).transpose(1, 0, 2)
        partial_value = lax.map(project_leaf, (rounded, basis_rows))
        groups = leaves // (2 ** height)
        node_total = partial_value.reshape(groups, 2 ** height, RHS, 2, RANK).sum(axis=1)
        node_total = jnp.moveaxis(node_total, 2, 1)
        half_count = 2 ** (height - 1)
        coefficient = jnp.broadcast_to(node_total[:, :, None], (groups, 2, half_count, RHS, RANK))
        coefficient = coefficient.reshape(leaves, RHS, RANK).astype(jnp.bfloat16)
        state = state - lax.map(leaf_apply, (coefficient, up_rows))
    return state.transpose(1, 0, 2).reshape(RHS, leaves * LEAF)
```

```python
import functools

import jax
import jax.numpy as jnp
from jax import lax
from jax.experimental import pallas as pl
from jax.experimental.pallas import tpu as pltpu
from jax.sharding import PartitionSpec as P

CHUNKS = 2
SUBLANES = 8
TILE = 256
F32 = jnp.float32
BF16 = jnp.bfloat16


def level_plan(height, bits_x, rows):
    top = height - 1
    groups = []
    low = [b for b in range(min(top, bits_x))]
    high = [b for b in range(bits_x, top)]
    if top == bits_x:
        groups.append([top])
    elif top > bits_x:
        groups.append([bits_x])
        groups.append([top] + high[1:])
    if top < bits_x and len(low) < 2:
        groups.append(low + [top])
    else:
        while low:
            groups.append(low[:2])
            low = low[2:]
        if top < bits_x:
            groups.append([top])
    phases = []
    for bits in groups:
        split = [b for b in bits if b != top]
        if rows >> len(split) < SUBLANES:
            assert top not in bits
            phases.append(("sum", bits))
        else:
            rows >>= len(split)
            phases.append(("scatter", bits))
    return phases


def masks_of(bits):
    masks = [0]
    for b in bits:
        masks += [m | 1 << b for m in masks]
    return masks[1:]


def sub_index(pos, bits):
    index = 0
    for k, b in enumerate(bits):
        index = index + ((pos >> b) & 1) * (1 << k)
    return index


def build_plan(levels, bits_x, rows, rank):
    plan, shapes, sems = [], [], 0

    def buf(*shape):
        shapes.append(shape)
        return len(shapes) - 1

    for height in range(1, levels + 1):
        top = height - 1
        n, c = rows, 2
        source = buf(c, n, rank)
        steps = []
        for kind, bits in level_plan(height, bits_x, rows):
            masks = masks_of(bits)
            split = [b for b in bits if b != top] if kind == "scatter" else []
            n >>= len(split)
            if top in bits:
                c = 1
            landing = buf(len(masks), c, n, rank)
            result = buf(c, n, rank)
            steps.append((kind, bits, split, masks, source, landing, result, n, c, sems))
            sems += len(masks)
            source = result
        for _, bits, split, *_ in reversed(list(steps)):
            if not split:
                continue
            masks = masks_of(split)
            result = buf(1, n << len(split), rank)
            steps.append(("gather", split, split, masks, source, None, result, n, 1, sems))
            sems += len(masks)
            n <<= len(split)
            source = result
        plan.append(steps)
    return plan, shapes, sems


def kernel(dims, plan, rhs_hbm, leaf_hbm, up_hbm, proj_hbm, out_hbm, *scratch):
    bits_x, bits_y, levels, chunks, rows, points, rank = dims
    rhs, leaf, up, proj, state, rounded = scratch[:6]
    in_sems, out_sems, send_sems, recv_sems = scratch[6:10]
    per_chunk = (len(scratch) - 10) // chunks
    gx, gy = lax.axis_index("gx"), lax.axis_index("gy")
    pos = gy * (1 << bits_x) + gx

    def device(mask):
        return {"gx": gx ^ (mask & ((1 << bits_x) - 1)), "gy": gy ^ (mask >> bits_x)}

    loads = [
        pltpu.make_async_copy(rhs_hbm, rhs, in_sems.at[0]),
        pltpu.make_async_copy(leaf_hbm.at[0], leaf, in_sems.at[1]),
    ]
    for level in range(levels):
        loads.append(pltpu.make_async_copy(proj_hbm.at[level], proj.at[level], in_sems.at[2 + 2 * level]))
        loads.append(pltpu.make_async_copy(up_hbm.at[level], up.at[level], in_sems.at[3 + 2 * level]))
    for load in loads:
        load.start()

    everyone = set()
    for steps in plan:
        for step in steps:
            everyone.update(step[3])
    barrier = pltpu.get_barrier_semaphore()
    for mask in sorted(everyone):
        pl.semaphore_signal(barrier, inc=1, device_id=device(mask), device_id_type=pl.DeviceIdType.MESH)
    loads[0].wait()
    loads[1].wait()

    def leaf_apply(lo):
        @pl.loop(0, points // TILE)
        def _(tile):
            cols = pl.ds(pl.multiple_of(tile * TILE, TILE), TILE)
            value = jnp.dot(rhs[lo : lo + rows, :], leaf[:, cols], preferred_element_type=F32)
            state[lo : lo + rows, cols] = value
            rounded[lo : lo + rows, cols] = value.astype(BF16)

    def update(lo, level, coefficient):
        @pl.loop(0, points // TILE)
        def _(tile):
            cols = pl.ds(pl.multiple_of(tile * TILE, TILE), TILE)
            value = state[lo : lo + rows, cols] - jnp.dot(
                coefficient, up[level, :, cols], preferred_element_type=F32
            )
            state[lo : lo + rows, cols] = value
            rounded[lo : lo + rows, cols] = value.astype(BF16)

    leaf_apply(0)
    pl.semaphore_wait(barrier, len(everyone))

    def flow(chunk):
        lo = chunk * rows
        bufs = scratch[10 + chunk * per_chunk : 10 + (chunk + 1) * per_chunk]
        if chunk:
            leaf_apply(lo)
        sends = []
        for level in range(levels):
            top = level
            if chunk == 0:
                loads[2 + 2 * level].wait()
            whole = bufs[plan[level][0][4]]
            for half in range(2):
                whole[half] = lax.dot_general(
                    rounded[lo : lo + rows, :],
                    proj[level, half * rank : (half + 1) * rank, :],
                    (((1,), (1,)), ((), ())),
                    preferred_element_type=F32,
                )
            bit = (pos >> top) & 1
            for kind, bits, split, masks, src, landing, dst, n, c, sem in plan[level]:
                copies = []
                src_ref, dst_ref = bufs[src], bufs[dst]

                def piece(who):
                    row = pl.ds(pl.multiple_of(sub_index(who, split) * n, n), n)
                    if top in bits:
                        return pl.ds((who >> top) & 1, 1), row
                    return pl.ds(0, c), row

                if kind == "gather":
                    own = pl.ds(pl.multiple_of(sub_index(pos, split) * n, n), n)
                for k, mask in enumerate(masks):
                    if kind == "gather":
                        frm, to = src_ref, dst_ref.at[:, own]
                    else:
                        frm, to = src_ref.at[piece(pos ^ mask)], bufs[landing].at[k]
                    copy = pltpu.make_async_remote_copy(
                        src_ref=frm,
                        dst_ref=to,
                        send_sem=send_sems.at[chunk, sem + k],
                        recv_sem=recv_sems.at[chunk, sem + k],
                        device_id=device(mask),
                        device_id_type=pl.DeviceIdType.MESH,
                    )
                    copy.start()
                    copies.append(copy)
                sends += copies
                if kind == "gather":
                    dst_ref[:, own] = src_ref[...]
                yield
                if kind == "gather":
                    for copy in copies:
                        copy.wait_recv()
                else:
                    for copy in copies:
                        copy.wait_recv()
                    total = src_ref[piece(pos)]
                    for k in range(len(masks)):
                        total = total + bufs[landing][k]
                    dst_ref[...] = total
            coefficient = bufs[plan[level][-1][6]][0].astype(BF16)
            if chunk == 0:
                loads[3 + 2 * level].wait()
            update(lo, level, coefficient)
        store = pltpu.make_async_copy(
            state.at[lo : lo + rows], out_hbm.at[lo : lo + rows], out_sems.at[chunk]
        )
        store.start()
        for copy in sends:
            copy.wait_send()
        yield
        store.wait()

    flows = [flow(chunk) for chunk in range(chunks)]
    while flows:
        left = []
        for item in flows:
            try:
                next(item)
                left.append(item)
            except StopIteration:
                pass
        flows = left


def shards(rhs, leaf_inverse, up_basis, projection):
    bits_x = lax.axis_size("gx").bit_length() - 1
    bits_y = lax.axis_size("gy").bit_length() - 1
    levels, rank, points = up_basis.shape
    rows = rhs.shape[0] // CHUNKS
    plan, shapes, sems = build_plan(levels, bits_x, rows, rank)
    dims = (bits_x, bits_y, levels, CHUNKS, rows, points, rank)
    any_spec = pl.BlockSpec(memory_space=pl.ANY)
    return pl.pallas_call(
        functools.partial(kernel, dims, plan),
        out_shape=jax.ShapeDtypeStruct(rhs.shape, F32),
        in_specs=[any_spec] * 4,
        out_specs=any_spec,
        scratch_shapes=[
            pltpu.VMEM(rhs.shape, BF16),
            pltpu.VMEM(leaf_inverse.shape[1:], BF16),
            pltpu.VMEM(up_basis.shape, BF16),
            pltpu.VMEM(projection.shape, BF16),
            pltpu.VMEM(rhs.shape, F32),
            pltpu.VMEM(rhs.shape, BF16),
            pltpu.SemaphoreType.DMA((2 + 2 * levels,)),
            pltpu.SemaphoreType.DMA((CHUNKS,)),
            pltpu.SemaphoreType.DMA((CHUNKS, sems)),
            pltpu.SemaphoreType.DMA((CHUNKS, sems)),
        ]
        + [pltpu.VMEM(shape, F32) for _ in range(CHUNKS) for shape in shapes],
        compiler_params=pltpu.CompilerParams(
            collective_id=0, has_side_effects=True, vmem_limit_bytes=60 * 2**20
        ),
    )(rhs, leaf_inverse, up_basis, projection)


def solution(mesh):
    return jax.shard_map(
        shards,
        mesh=mesh,
        in_specs=(
            P(None, ("gy", "gx")),
            P(("gy", "gx"), None, None),
            P(None, None, ("gy", "gx")),
            P(None, None, ("gy", "gx")),
        ),
        out_specs=P(None, ("gy", "gx")),
        check_vma=False,
    )
```

```python
import functools

import jax
import jax.numpy as jnp
from jax import lax
from jax.experimental import pallas as pl
from jax.experimental.pallas import tpu as pltpu
from jax.sharding import PartitionSpec as P

CHUNKS = 2
SUBLANES = 8
TILE = 1024
F32 = jnp.float32
BF16 = jnp.bfloat16


def level_plan(height, bits_x, rows):
    top = height - 1
    groups = []
    low = [b for b in range(min(top, bits_x))]
    high = [b for b in range(bits_x, top)]
    if top == bits_x:
        groups.append([top])
    elif top > bits_x:
        groups.append([bits_x])
        last = [top] + high[1:]
        if len(low) <= 3 and rows >> len(low) + len(high) >= SUBLANES:
            last, low = last + low, []
        groups.append(last)
    if top < bits_x and len(low) < 3:
        groups.append(low + [top])
    else:
        while low:
            groups.append(low[:3])
            low = low[3:]
        if top < bits_x:
            groups.append([top])
    phases = []
    for bits in groups:
        split = [b for b in bits if b != top]
        if rows >> len(split) < SUBLANES:
            assert top not in bits
            phases.append(("sum", bits))
        else:
            rows >>= len(split)
            phases.append(("scatter", bits))
    return phases


def masks_of(bits):
    masks = [0]
    for b in bits:
        masks += [m | 1 << b for m in masks]
    return masks[1:]


def sub_index(pos, bits):
    index = 0
    for k, b in enumerate(bits):
        index = index + ((pos >> b) & 1) * (1 << k)
    return index


def build_plan(levels, bits_x, rows, rank):
    plan, shapes, sems = [], [], 0

    def buf(*shape):
        shapes.append(shape)
        return len(shapes) - 1

    for height in range(1, levels + 1):
        top = height - 1
        n, c = rows, 2
        source = buf(c, n, rank)
        steps = []
        for kind, bits in level_plan(height, bits_x, rows):
            masks = masks_of(bits)
            split = [b for b in bits if b != top] if kind == "scatter" else []
            n >>= len(split)
            if top in bits:
                c = 1
            landing = buf(len(masks), c, n, rank)
            result = buf(c, n, rank)
            steps.append((kind, bits, split, masks, source, landing, result, n, c, sems))
            sems += len(masks)
            source = result
        for _, bits, split, *_ in reversed(list(steps)):
            if not split:
                continue
            masks = masks_of(split)
            result = buf(1, n << len(split), rank)
            steps.append(("gather", split, split, masks, source, None, result, n, 1, sems))
            sems += len(masks)
            n <<= len(split)
            source = result
        plan.append(steps)
    return plan, shapes, sems


def kernel(dims, plan, rhs_hbm, leaf_hbm, up_hbm, proj_hbm, out_hbm, last_ref, *scratch):
    bits_x, bits_y, levels, chunks, rows, points, rank = dims
    rhs, leaf, up, proj, state, rounded = scratch[:6]
    in_sems, out_sems, send_sems, recv_sems = scratch[6:10]
    per_chunk = (len(scratch) - 10) // chunks
    gx, gy = lax.axis_index("gx"), lax.axis_index("gy")
    pos = gy * (1 << bits_x) + gx

    def device(mask):
        return {"gx": gx ^ (mask & ((1 << bits_x) - 1)), "gy": gy ^ (mask >> bits_x)}

    loads = [
        pltpu.make_async_copy(rhs_hbm, rhs, in_sems.at[0]),
        pltpu.make_async_copy(leaf_hbm.at[0], leaf, in_sems.at[1]),
    ]
    for level in range(levels):
        loads.append(pltpu.make_async_copy(proj_hbm.at[level], proj.at[level], in_sems.at[2 + 2 * level]))
        if level < levels - 1:
            loads.append(pltpu.make_async_copy(up_hbm.at[level], up.at[level], in_sems.at[3 + 2 * level]))
    for load in loads:
        load.start()

    everyone = set()
    for steps in plan:
        for step in steps:
            everyone.update(step[3])
    barrier = pltpu.get_barrier_semaphore()
    for mask in sorted(everyone):
        pl.semaphore_signal(barrier, inc=1, device_id=device(mask), device_id_type=pl.DeviceIdType.MESH)
    loads[0].wait()
    loads[1].wait()

    def leaf_apply(lo):
        @pl.loop(0, points // TILE)
        def _(tile):
            cols = pl.ds(pl.multiple_of(tile * TILE, TILE), TILE)
            value = jnp.dot(rhs[lo : lo + rows, :], leaf[:, cols], preferred_element_type=F32)
            state[lo : lo + rows, cols] = value
            rounded[lo : lo + rows, cols] = value.astype(BF16)

    def update(lo, level, coefficient):
        @pl.loop(0, points // TILE)
        def _(tile):
            cols = pl.ds(pl.multiple_of(tile * TILE, TILE), TILE)
            value = state[lo : lo + rows, cols] - jnp.dot(
                coefficient, up[level, :, cols], preferred_element_type=F32
            )
            state[lo : lo + rows, cols] = value
            rounded[lo : lo + rows, cols] = value.astype(BF16)

    leaf_apply(0)
    pl.semaphore_wait(barrier, len(everyone))

    def flow(chunk):
        lo = chunk * rows
        bufs = scratch[10 + chunk * per_chunk : 10 + (chunk + 1) * per_chunk]
        if chunk:
            leaf_apply(lo)
        sends = []
        for level in range(levels):
            top = level
            if chunk == 0:
                loads[2 + 2 * level].wait()
            whole = bufs[plan[level][0][4]]
            for half in range(2):
                whole[half] = lax.dot_general(
                    rounded[lo : lo + rows, :],
                    proj[level, half * rank : (half + 1) * rank, :],
                    (((1,), (1,)), ((), ())),
                    preferred_element_type=F32,
                )
            bit = (pos >> top) & 1
            for kind, bits, split, masks, src, landing, dst, n, c, sem in plan[level]:
                copies = []
                src_ref, dst_ref = bufs[src], bufs[dst]

                def piece(who):
                    row = pl.ds(pl.multiple_of(sub_index(who, split) * n, n), n)
                    if top in bits:
                        return pl.ds((who >> top) & 1, 1), row
                    return pl.ds(0, c), row

                if kind == "gather":
                    own = pl.ds(pl.multiple_of(sub_index(pos, split) * n, n), n)
                for k, mask in enumerate(masks):
                    if kind == "gather":
                        frm, to = src_ref, dst_ref.at[:, own]
                    else:
                        frm, to = src_ref.at[piece(pos ^ mask)], bufs[landing].at[k]
                    copy = pltpu.make_async_remote_copy(
                        src_ref=frm,
                        dst_ref=to,
                        send_sem=send_sems.at[chunk, sem + k],
                        recv_sem=recv_sems.at[chunk, sem + k],
                        device_id=device(mask),
                        device_id_type=pl.DeviceIdType.MESH,
                    )
                    copy.start()
                    copies.append(copy)
                sends += copies
                if kind == "gather":
                    dst_ref[:, own] = src_ref[...]
                yield
                if kind == "gather":
                    for copy in copies:
                        copy.wait_recv()
                else:
                    for copy in copies:
                        copy.wait_recv()
                    total = src_ref[piece(pos)]
                    for k in range(len(masks)):
                        total = total + bufs[landing][k]
                    dst_ref[...] = total
            coefficient = bufs[plan[level][-1][6]][0].astype(BF16)
            if level == levels - 1:
                last_ref[lo : lo + rows, :] = coefficient
                break
            if chunk == 0:
                loads[3 + 2 * level].wait()
            update(lo, level, coefficient)
            if level == levels - 2:
                store = pltpu.make_async_copy(
                    state.at[lo : lo + rows], out_hbm.at[lo : lo + rows], out_sems.at[chunk]
                )
                store.start()
        for copy in sends:
            copy.wait_send()
        yield
        store.wait()

    flows = [flow(chunk) for chunk in range(chunks)]
    while flows:
        left = []
        for item in flows:
            try:
                next(item)
                left.append(item)
            except StopIteration:
                pass
        flows = left


def shards(rhs, leaf_inverse, up_basis, projection):
    bits_x = lax.axis_size("gx").bit_length() - 1
    bits_y = lax.axis_size("gy").bit_length() - 1
    levels, rank, points = up_basis.shape
    rows = rhs.shape[0] // CHUNKS
    plan, shapes, sems = build_plan(levels, bits_x, rows, rank)
    dims = (bits_x, bits_y, levels, CHUNKS, rows, points, rank)
    any_spec = pl.BlockSpec(memory_space=pl.ANY)
    state, coefficient = pl.pallas_call(
        functools.partial(kernel, dims, plan),
        out_shape=(
            jax.ShapeDtypeStruct(rhs.shape, F32),
            jax.ShapeDtypeStruct((rhs.shape[0], rank), BF16),
        ),
        in_specs=[any_spec] * 4,
        out_specs=(any_spec, pl.BlockSpec(memory_space=pltpu.VMEM)),
        scratch_shapes=[
            pltpu.VMEM(rhs.shape, BF16),
            pltpu.VMEM(leaf_inverse.shape[1:], BF16),
            pltpu.VMEM(up_basis.shape, BF16),
            pltpu.VMEM(projection.shape, BF16),
            pltpu.VMEM(rhs.shape, F32),
            pltpu.VMEM(rhs.shape, BF16),
            pltpu.SemaphoreType.DMA((2 + 2 * levels,)),
            pltpu.SemaphoreType.DMA((CHUNKS,)),
            pltpu.SemaphoreType.DMA((CHUNKS, sems)),
            pltpu.SemaphoreType.DMA((CHUNKS, sems)),
        ]
        + [pltpu.VMEM(shape, F32) for _ in range(CHUNKS) for shape in shapes],
        compiler_params=pltpu.CompilerParams(
            collective_id=0, has_side_effects=True, vmem_limit_bytes=60 * 2**20
        ),
    )(rhs, leaf_inverse, up_basis, projection)
    return state - jnp.dot(coefficient, up_basis[levels - 1], preferred_element_type=F32)


def solution(mesh):
    return jax.shard_map(
        shards,
        mesh=mesh,
        in_specs=(
            P(None, ("gy", "gx")),
            P(("gy", "gx"), None, None),
            P(None, None, ("gy", "gx")),
            P(None, None, ("gy", "gx")),
        ),
        out_specs=P(None, ("gy", "gx")),
        check_vma=False,
    )
```
